32 devices in a mesh: det: 8 (over z, y), row: 4 (over x, core).
Axes of the slice: x: 2, y: 2, z: 4, core: 2. Of those that a mesh axis runs over, the one named last changes fastest.
Arguments:
- science: float32 [8, 128, 768], P('det', 'row'), may hold values from -6 to 6
- template: float32 [8, 6, 128, 128], P('det', None, 'row'), may hold values from -6 to 6
- tile_source: int32 [8, 6], replicated, may hold values from 0 to 47, as said below
- offsets: int32 [2, 8, 6], P(None, 'det'), may hold values from 0 to 3
- shift_weights: float32 [2, 8, 6], P(None, 'det'), may hold values from 0 to 1
- valid_rows: int32 [8, 6], P('det'), may hold values from 32 to 128
- basis_kernels: float32 [27, 31, 31], replicated, may hold values from -0.1875 to 0.1875
- coefficients: float32 [8, 27], P('det'), may hold values from -1.25 to 1.25
- background: float32 [8], P('det'), may hold values from -4 to 4
Outputs:
- difference_tiles: float32 [8, 6, 128, 128], P('det', None, 'row')
The draws below stay inside these ranges and needn't reach their ends.
Inputs may be any that keep to these rules, and one draw needn't show every extreme that they name: `tile_source`: entry [d, c] names slot s of sky patch p as p * 6 + s. Row d names the patches (d + j) mod 8 for j = 0 .. 3, in that order along the columns, each in one run of consecutive columns that names consecutive slots, 1 to 3 tiles long; one run of each row is exactly 3 long.
All inputs are finite; a program needn't handle non-finite values.
Results may differ from the reference program's by a relative error of at most 0.000062.
Values sent between devices are 32-bit elements; how exact they have to be, the bound alone decides.
No kernel may reach another device: no remote copies, remote signals or barrier semaphores. Data moves between devices by JAX's collectives and lax.ppermute only.
A program may use at most 64 MiB of HBM per device.

```python
import jax
import jax.numpy as jnp
from jax import lax

TILE = 128
TC = 6
KW = 31
NB = 27
MAXOFF = 4
SPAN = 4
DETS = 8
W = 768
PT_DEV = 6
CAP = 3
HALF = 15


def route_table(key):
    first_key, second_key, third_key, fourth_key = jax.random.split(jax.random.fold_in(key, 7), 4)
    lower_cut = jax.random.randint(first_key, (DETS,), 1, CAP - 1).astype(jnp.int32)
    upper_cut = jax.random.randint(second_key, (DETS,), lower_cut + 1, CAP).astype(jnp.int32)
    remaining = jnp.stack([lower_cut, upper_cut - lower_cut, CAP - upper_cut], axis=1).astype(jnp.int32)
    longest = jax.random.randint(third_key, (DETS, 1), 0, SPAN).astype(jnp.int32)
    run_ids = jnp.arange(SPAN, dtype=jnp.int32)[None, :]
    rest_index = jnp.clip(run_ids - (run_ids > longest).astype(jnp.int32), 0, SPAN - 2)
    runs = jnp.where(run_ids == longest, jnp.int32(CAP), jnp.take_along_axis(remaining, rest_index, axis=1)).astype(jnp.int32)
    ends = jnp.cumsum(runs, axis=1).astype(jnp.int32)
    starts = (ends - runs).astype(jnp.int32)
    column_ids = jnp.arange(TC, dtype=jnp.int32)
    run_of = jnp.sum((column_ids[None, :, None] >= ends[:, None, :SPAN - 1]).astype(jnp.int32), axis=2).astype(jnp.int32)
    ranks = column_ids[None, :] - jnp.take_along_axis(starts, run_of, axis=1)
    slot_start = jax.random.randint(fourth_key, (DETS, SPAN), 0, PT_DEV - runs + 1).astype(jnp.int32)
    slots = jnp.take_along_axis(slot_start, run_of, axis=1) + ranks
    owners = (jnp.arange(DETS, dtype=jnp.int32)[:, None] + run_of) % DETS
    return (owners * PT_DEV + slots).astype(jnp.int32)


def draw_tile_source(key, part):
    return route_table(key)


def set_ends(values, stream_key, low, top_value):
    index_at = [jax.random.randint(jax.random.fold_in(stream_key, axis), (), 0, length) for axis, length in enumerate(values.shape)]
    main_axis = values.shape.index(max(values.shape))
    next_to = index_at[:main_axis] + [(index_at[main_axis] + 1) % values.shape[main_axis]] + index_at[main_axis + 1:]
    return values.at[tuple(index_at)].set(low).at[tuple(next_to)].set(top_value)


def shard_levels(stream_key, shape, cuts, least, largest):
    def one(axis_at, shards_of):
        draws = jax.random.uniform(jax.random.fold_in(jax.random.fold_in(stream_key, 6), axis_at), (shards_of,), jnp.float32, least / len(cuts), largest / len(cuts))
        return jnp.repeat(jnp.exp(draws), shape[axis_at] // shards_of).reshape((-1,) + (1,) * (len(shape) - axis_at - 1))

    level = one(*cuts[0])
    for cut in cuts[1:]:
        level = level * one(*cut)
    return level


def scatter_about(rng, dims, width, bound, shards=(), kind=jnp.bfloat16):
    factor_of = shard_levels(rng, dims, shards, -0.22, 0.18) if shards else 1.0
    values = jax.random.normal(rng, dims, jnp.float32) * width * factor_of
    return jnp.minimum(jnp.maximum(values, -bound), bound).astype(kind)


def setup_inputs(seed: int = 0) -> dict:
    keys = jax.random.split(jax.random.key(seed), 10)
    science = scatter_about(keys[0], (DETS, TILE, W), 1.0, 6.0, ((0, 8), (1, 4)), jnp.float32)
    template = scatter_about(keys[1], (DETS, PT_DEV, TILE, TILE), 1.0, 6.0, ((0, 8), (2, 4)), jnp.float32)
    tile_source = draw_tile_source(jax.random.fold_in(keys[9], 71), 0)
    offsets = set_ends(jax.random.randint(keys[3], (2, DETS, TC), 0, MAXOFF), jax.random.fold_in(keys[3], 1), 0, MAXOFF - 1).astype(jnp.int32)
    shift_weights = jnp.clip(1.0 * jax.random.uniform(keys[4], (2, DETS, TC), jnp.float32) ** shard_levels(keys[4], (2, DETS, TC), ((1, 8),), -0.2, 0.2), 0.0, 1.0)
    valid_rows = set_ends(jax.random.randint(keys[5], (DETS, TC), TILE // 4, TILE + 1), jax.random.fold_in(keys[5], 1), TILE // 4, TILE).astype(jnp.int32)
    basis_kernels = scatter_about(keys[6], (NB, KW, KW), (KW * KW) ** -0.5, 0.1875, (), jnp.float32)
    coefficients = scatter_about(keys[7], (DETS, NB), NB ** -0.5, 1.25, ((0, 8),), jnp.float32)
    background = scatter_about(keys[8], (DETS,), 1.0, 4.0, ((0, 8),), jnp.float32)
    return dict(science=science, template=template, tile_source=tile_source, offsets=offsets, shift_weights=shift_weights, valid_rows=valid_rows, basis_kernels=basis_kernels, coefficients=coefficients, background=background)


def convolve(pair):
    image, kernel = pair
    result = lax.conv_general_dilated(image[None, None], kernel[None, None], (1, 1), ((HALF, HALF), (HALF, HALF)), precision=lax.Precision.HIGHEST)
    return result[0, 0]


def reference(science, template, tile_source, offsets, shift_weights, valid_rows, basis_kernels, coefficients, background):
    flat_tiles = template.reshape(DETS * PT_DEV, TILE, TILE)
    sources = tile_source.reshape(-1).astype(jnp.int32)
    gathered = flat_tiles[sources]
    row_shift = offsets[0].reshape(-1).astype(jnp.int32)
    column_shift = offsets[1].reshape(-1).astype(jnp.int32)
    row_weight = shift_weights[0].reshape(-1)
    column_weight = shift_weights[1].reshape(-1)
    column_ids = jnp.arange(TILE, dtype=jnp.int32)
    first_cols = jnp.minimum(column_ids[None, :] + column_shift[:, None], TILE - 1)
    second_cols = jnp.minimum(column_ids[None, :] + column_shift[:, None] + 1, TILE - 1)
    left_part = jnp.take_along_axis(gathered, first_cols[:, None, :], axis=2)
    right_part = jnp.take_along_axis(gathered, second_cols[:, None, :], axis=2)
    across = (1.0 - column_weight)[:, None, None] * left_part + column_weight[:, None, None] * right_part
    padded = jnp.pad(across, ((0, 0), (0, MAXOFF + 1), (0, 0)))
    first_rows = column_ids[None, :] + row_shift[:, None]
    upper_part = jnp.take_along_axis(padded, first_rows[:, :, None], axis=1)
    lower_part = jnp.take_along_axis(padded, first_rows[:, :, None] + 1, axis=1)
    warped = (1.0 - row_weight)[:, None, None] * upper_part + row_weight[:, None, None] * lower_part
    warped = warped.reshape(DETS, TC, TILE, TILE).transpose(0, 2, 1, 3).reshape(DETS, TILE, W)
    kernels = jnp.einsum('dk,kab->dab', coefficients, basis_kernels, precision=lax.Precision.HIGHEST)
    modelled = lax.map(convolve, (warped, kernels))
    residual_image = science - modelled - background[:, None, None]
    limits = jnp.repeat(valid_rows.astype(jnp.int32), TILE, axis=1)
    inside = column_ids[None, :, None] < limits[:, None, :]
    residual_image = jnp.where(inside, residual_image, jnp.float32(0.0))
    pieces = residual_image.reshape(DETS, TILE, TC, TILE).transpose(0, 2, 1, 3).reshape(DETS * TC, TILE, TILE)
    summed = jax.ops.segment_sum(pieces, sources, num_segments=DETS * PT_DEV)
    tallies = jax.ops.segment_sum(jnp.ones(sources.shape, jnp.float32), sources, num_segments=DETS * PT_DEV)
    result = summed / jnp.maximum(tallies, 1.0)[:, None, None]
    return result.reshape(DETS, PT_DEV, TILE, TILE)
```

```python
import jax
import jax.numpy as jnp
from jax import lax
from jax.experimental import pallas as pl
from jax.experimental.pallas import tpu as pltpu
from jax.sharding import PartitionSpec as P

SPAN = 4
LONG = 3
LANES = 128
ABOVE = 16
BELOW = 24
EDGE = 32
SPLIT = 8


def fdiv(value, divisor, bound):
    factor = 65536 // divisor + 1
    assert bound * (factor * divisor - 65536) < 65536
    return (value * factor) >> 16


def run_info(sources, row, slots, dets):
    columns = sources.shape[1]
    reach = []
    for c in range(columns):
        owner = fdiv(sources[row, c], slots, dets * slots)
        step = owner - row
        reach.append(jnp.where(step < 0, step + dets, step))
    starts, lengths = [], []
    for j in range(SPAN):
        starts.append(sum((x < j).astype(jnp.int32) for x in reach))
        lengths.append(sum((x == j).astype(jnp.int32) for x in reach))
    return starts, lengths


def wrap(value, count):
    return jnp.where(value < 0, value + count, value)


def lane_ids(rows):
    return lax.broadcasted_iota(jnp.int32, (rows, LANES), 1)


def row_ids(rows):
    return lax.broadcasted_iota(jnp.int32, (rows, LANES), 0)


def prep_body(dets, where, src, off, sw, valid, coef, back, sci, tmpl, basis,
              out_a, out_b, out_3, out_2, out_0, halo_a, halo_b, kern):
    d = where[0]
    r = where[1]
    slots, band = tmpl.shape[0], tmpl.shape[1]
    columns = src.shape[1]
    even_d = lax.rem(d, 2) == 0
    even_r = lax.rem(r, 2) == 0
    starts, lengths = run_info(src, d, slots, dets)
    grow = row_ids(band) + r * band

    tiles = []
    for j in range(SPAN):
        mine = []
        for k in range(LONG):
            c = jnp.minimum(starts[j] + k, columns - 1)
            limit = jnp.where(k < lengths[j], valid[0, c], 0)
            block = sci[:, pl.ds(pl.multiple_of(c * LANES, LANES), LANES)]
            mine.append(jnp.where(grow < limit, block - back[0], 0.0))
        tiles.append(mine)

    width = basis.shape[1]
    total = coef[0, 0] * basis[0]
    for k in range(1, basis.shape[0]):
        total = total + coef[0, k] * basis[k]
    kern[...] = jnp.zeros_like(kern)
    kern[0:width, 0:width] = total
    flip = jnp.transpose(kern[...])
    packed = flip[0:8]
    for g in range(1, 4):
        packed = packed + pltpu.roll(flip[8 * g:8 * g + 8], EDGE * g, 1)

    lane8 = lane_ids(8)
    row8 = row_ids(8)
    params = jnp.zeros((8, LANES), jnp.float32)
    for c in range(columns):
        line = jnp.where(lane8 == 0, off[0, 0, c].astype(jnp.float32), 0.0)
        line = jnp.where(lane8 == 1, off[1, 0, c].astype(jnp.float32), line)
        line = jnp.where(lane8 == 2, sw[0, 0, c], line)
        line = jnp.where(lane8 == 3, sw[1, 0, c], line)
        line = jnp.where(lane8 == 4, valid[0, c].astype(jnp.float32), line)
        params = jnp.where(row8 == c, line, params)

    lane = lane_ids(band)
    left = jnp.zeros((band, LANES), jnp.float32)
    right = jnp.zeros((band, LANES), jnp.float32)
    for q in range(SPAN - 1):
        other = wrap(d - q, dets)
        st, ln = run_info(src, other, slots, dets)
        s = src[other, st[q] + ln[q] - 1] - d * slots
        piece = pltpu.roll(tmpl[s], (EDGE * q + EDGE) % LANES, 1)
        left = jnp.where((lane >= EDGE * q) & (lane < EDGE * q + EDGE), piece, left)
        other = wrap(d - q - 1, dets)
        st, ln = run_info(src, other, slots, dets)
        s = src[other, st[q + 1]] - d * slots
        piece = tmpl[s]
        if q:
            piece = pltpu.roll(piece, EDGE * q, 1)
        right = jnp.where((lane >= EDGE * q) & (lane < EDGE * q + EDGE), piece, right)

    def fill(ref, j):
        for k in range(LONG):
            ref[band * k:band * k + band] = tiles[j][k]
        ref[band * LONG:band * LONG + 8] = packed
        ref[band * LONG + 8:band * LONG + 16] = params

    fill(out_0, 0)
    fill(out_2, 2)
    fill(out_3, 3)

    def pair(plus, minus):
        fill(plus, 1)
        plus[band * LONG + 16:band * LONG + 16 + band] = left
        minus[0:band * LONG + 16] = jnp.zeros((band * LONG + 16, LANES), jnp.float32)
        minus[band * LONG + 16:band * LONG + 16 + band] = right

    @pl.when(even_d)
    def _():
        pair(out_a, out_b)

    @pl.when(jnp.logical_not(even_d))
    def _():
        pair(out_b, out_a)

    for s in range(slots):
        top = tmpl[s, 0:BELOW]
        bottom = tmpl[s, band - BELOW:band]
        halo_a[:, LANES * s:LANES * s + LANES] = jnp.where(even_r, bottom, top)
        halo_b[:, LANES * s:LANES * s + LANES] = jnp.where(even_r, top, bottom)


def pack_body(band, slots, where, got_a, got_b, in_a, in_b, halo_a, halo_b):
    halo_a[:, 0:LANES * slots] = in_a[...]
    halo_b[:, 0:LANES * slots] = in_b[...]
    d = where[0]
    r = where[1]
    even_d = lax.rem(d, 2) == 0
    even_r = lax.rem(r, 2) == 0
    base = got_a.shape[0] - band
    from_a = got_a[base:base + band]
    from_b = got_b[base:base + band]
    left = jnp.where(even_d, from_b, from_a)
    right = jnp.where(even_d, from_a, from_b)
    for i, strip in enumerate((left, right)):
        at = LANES * (slots + i)
        top = strip[0:BELOW]
        bottom = strip[band - BELOW:band]
        halo_a[:, at:at + LANES] = jnp.where(even_r, bottom, top)
        halo_b[:, at:at + LANES] = jnp.where(even_r, top, bottom)


def main_body(dets, where, src, tmpl, own, got_a, got_b, got_2, got_3, halo_a, halo_b, out,
              plus, minus, scal, sem, tiles, lefts, rights, kpad, rho, vmat, ws, wt, acc, sacc, tr):
    d = where[0]
    r = where[1]
    slots, band = tmpl.shape[0], tmpl.shape[1]
    columns = src.shape[1]
    even_d = lax.rem(d, 2) == 0
    even_r = lax.rem(r, 2) == 0
    base = got_a.shape[0] - band
    tpad = LANES + 8
    spad = EDGE + 8

    @pl.when(even_d)
    def _():
        plus[...] = got_b[...]
        minus[...] = got_a[base:base + band]

    @pl.when(jnp.logical_not(even_d))
    def _():
        plus[...] = got_a[...]
        minus[...] = got_b[base:base + band]

    packets = [own, plus, got_2, got_3]
    copies = []
    for j in range(SPAN):
        copies.append(pltpu.make_async_copy(
            packets[j].at[pl.ds(band * LONG + 8, 8), :], scal.at[j], sem.at[j]))
        copies[-1].start()

    def stacked(middle, at):
        up_a = halo_a[BELOW - ABOVE:BELOW, at:at + LANES]
        up_b = halo_b[BELOW - ABOVE:BELOW, at:at + LANES]
        dn_a = halo_a[:, at:at + LANES]
        dn_b = halo_b[:, at:at + LANES]
        up = jnp.where(even_r, up_b, up_a)
        down = jnp.where(even_r, dn_a, dn_b)
        return jnp.transpose(jnp.concatenate([up, middle, down], axis=0))

    tall = ABOVE + band + BELOW
    for s in range(slots):
        t = stacked(tmpl[s], LANES * s)
        tiles[tpad * s:tpad * s + LANES, 0:tall] = t
        tiles[tpad * s + LANES:tpad * s + tpad, 0:tall] = jnp.broadcast_to(t[LANES - 1:LANES], (8, tall))
    t = stacked(plus[base:base + band], LANES * slots)
    for q in range(SPAN - 1):
        lefts[spad * q:spad * q + EDGE, 0:tall] = t[EDGE * q:EDGE * q + EDGE]
        lefts[spad * q + EDGE:spad * q + spad, 0:tall] = jnp.broadcast_to(
            t[EDGE * q + EDGE - 1:EDGE * q + EDGE], (8, tall))
    rights[:, 0:tall] = stacked(minus[...], LANES * (slots + 1))

    lane = lane_ids(8)
    kpad[...] = jnp.zeros_like(kpad)
    for j in range(SPAN):
        pk = packets[j][band * LONG:band * LONG + 8]
        back = (EDGE - lane // 4) % EDGE
        for g in range(4):
            kpad[8 + 8 * g:16 + 8 * g] = jnp.take_along_axis(pk, back + EDGE * g, axis=1)
        line = jnp.zeros((40, LANES), jnp.float32)
        dx = lane_ids(40) % 4
        for k in range(4):
            line = jnp.where(dx == k, kpad[8 - k:48 - k], line)
        rho[...] = line
        keep = (lane_ids(EDGE) // 4) <= row_ids(EDGE)
        for u in range(36):
            one = jnp.broadcast_to(rho[u:u + 1], (EDGE, LANES))
            one = pltpu.roll(one, 0, 1, stride=4, stride_axis=0)
            high = one.astype(jnp.bfloat16).astype(jnp.float32)
            low = one - high
            at = 64 * u
            vmat[j, at:at + EDGE, 0:LANES] = jnp.where(keep, high, 0.0).astype(jnp.bfloat16)
            vmat[j, at + EDGE:at + 64, 0:LANES] = jnp.where(keep, 0.0, high).astype(jnp.bfloat16)
            vmat[j, at:at + EDGE, LANES:2 * LANES] = jnp.where(keep, low, 0.0).astype(jnp.bfloat16)
            vmat[j, at + EDGE:at + 64, LANES:2 * LANES] = jnp.where(keep, 0.0, low).astype(jnp.bfloat16)

    acc[...] = jnp.zeros_like(acc)
    sacc[...] = jnp.zeros_like(sacc)
    ws[...] = jnp.zeros_like(ws)
    for c in copies:
        c.wait()

    def warp(j, c, ref, at, count, dst):
        ro = scal[j, c, 0].astype(jnp.int32)
        co = scal[j, c, 1].astype(jnp.int32)
        rw = scal[j, c, 2]
        cw = scal[j, c, 3]
        one = ref[pl.ds(at + co, count), :]
        two = ref[pl.ds(at + co + 1, count), :]
        mix = (1.0 - cw) * one + cw * two
        upper = pltpu.roll(mix, LANES - 1 - ro, 1)
        lower = pltpu.roll(mix, LANES - 2 - ro, 1)
        both = (1.0 - rw) * upper + rw * lower
        ids = lane_ids(count)
        grow = ids + (r * band - (ABOVE - 1))
        ok = (ids < 64) & (grow >= 0) & (grow < LANES)
        ws[pl.ds(dst, count), :] = jnp.where(ok, both, 0.0)

    def conv(j, rows):
        total = jnp.zeros((2 * rows, 2 * LANES), jnp.float32)
        for t in range(9):
            one = wt[pl.ds(9 + 4 * t, rows, stride=4), :]
            two = wt[pl.ds(11 + 4 * t, rows, stride=4), :]
            lhs = jnp.concatenate([one, two], axis=1)
            high = lhs.astype(jnp.bfloat16)
            low = (lhs - high.astype(jnp.float32)).astype(jnp.bfloat16)
            total = total + jnp.dot(
                jnp.concatenate([high, low], axis=0), vmat[j, 256 * t:256 * t + 256],
                preferred_element_type=jnp.float32)
        res = total[0:rows] + total[rows:2 * rows]
        return res[:, 0:LANES] + res[:, LANES:2 * LANES]

    tally = [jnp.int32(0) for _ in range(slots)]
    for j in range(SPAN):
        det = wrap(d - j, dets)
        st, ln = run_info(src, det, slots, dets)
        st, ln = st[j], ln[j]
        s0 = src[det, st] - d * slots
        for s in range(slots):
            tally[s] = tally[s] + ((s0 <= s) & (s < s0 + ln)).astype(jnp.int32)
        if j > 0:
            warp(j, st - 1, lefts, spad * (j - 1) + EDGE - 16, 16, 8)
        else:
            ws[8:24] = jnp.zeros((16, LANES), jnp.float32)
        end = pl.multiple_of(24 + LANES * ln, 8)
        if j < SPAN - 1:
            warp(j, jnp.minimum(st + ln, columns - 1), rights, EDGE * j, 16, end)
        else:
            ws[pl.ds(end, 16), :] = jnp.zeros((16, LANES), jnp.float32)

        def finish(count, j=j, st=st, s0=s0):
            for k in range(count):
                warp(j, st + k, tiles, (s0 + k) * tpad, LANES, 24 + LANES * k)
            n = LANES * count + 40
            wt[pl.ds(8, n), :] = ws[pl.ds(8, n), :] + pltpu.roll(ws[pl.ds(9, n), :], 64, 1)
            res = conv(j, EDGE * count)
            ids = lane_ids(EDGE) // 4 + r * band
            for k in range(count):
                limit = scal[j, st + k, 4].astype(jnp.int32)
                piece = jnp.where(ids < limit, res[EDGE * k:EDGE * k + EDGE], 0.0)
                at = pl.multiple_of((s0 + k) * EDGE, EDGE)
                acc[pl.ds(at, EDGE), :] += piece
                sacc[pl.ds(at, EDGE), :] += packets[j][band * k:band * k + band]

        @pl.when(ln == 1)
        def _():
            finish(1)

        @pl.when(ln != 1)
        def _():
            finish(LONG)

    for g in range(0, slots, 4):
        tr[...] = jnp.transpose(acc[EDGE * g:EDGE * g + LANES])
        planes = [tr[pl.ds(k, EDGE, stride=4), :] for k in range(4)]
        ids = lane_ids(EDGE)
        for s in range(g, min(g + 4, slots)):
            pick = ids // 4 + EDGE * (s - g)
            image = jnp.zeros((EDGE, LANES), jnp.float32)
            for k in range(4):
                image = jnp.where(ids % 4 == k, jnp.take_along_axis(planes[k], pick, axis=1), image)
            scale = jnp.float32(1.0)
            for n in range(2, SPAN + 1):
                scale = jnp.where(tally[s] == n, jnp.float32(1.0 / n), scale)
            out[s] = (sacc[EDGE * s:EDGE * s + EDGE] - image) * scale


def shifted(value, axis, steps):
    count = lax.axis_size(axis)
    return lax.ppermute(value, axis, [(i, (i + steps) % count) for i in range(count)])


def paired(value, axis, first, ring):
    count = lax.axis_size(axis)
    pairs = []
    for i in range(first, count if ring else count - 1, 2):
        k = (i + 1) % count
        pairs += [(i, k), (k, i)]
    return lax.ppermute(value, axis, pairs)


def body(science, template, tile_source, offsets, shift_weights, valid_rows, basis_kernels,
         coefficients, background):
    f32 = jnp.float32
    dets = lax.axis_size("det")
    assert dets % 2 == 0 and dets >= SPAN
    slots, band, tile = template.shape[1:]
    assert tile == LANES and band == EDGE
    where = jnp.stack([lax.axis_index("det"), lax.axis_index("row")]).astype(jnp.int32)
    vm = pl.BlockSpec(memory_space=pltpu.VMEM)
    sm = pl.BlockSpec(memory_space=pltpu.SMEM)
    rows = band * LONG + 16
    shapes = [(rows + band, LANES)] * 2 + [(rows, LANES)] * 3 + [(BELOW, LANES * slots)] * 2
    out_a, out_b, out_3, out_2, own, halo_a, halo_b = pl.pallas_call(
        lambda *refs: prep_body(dets, *refs),
        out_shape=[jax.ShapeDtypeStruct(s, f32) for s in shapes],
        in_specs=[sm] * 7 + [vm] * 3,
        out_specs=[vm] * len(shapes),
        scratch_shapes=[pltpu.VMEM((LANES, LANES), f32)],
        name="prep",
    )(where, tile_source, offsets, shift_weights, valid_rows, coefficients, background,
      science[0], template[0], basis_kernels)
    got_b = paired(out_b, "det", 1, True)
    got_a = paired(out_a, "det", 0, False)
    got_3 = shifted(out_3, "det", 3)
    got_2 = shifted(out_2, "det", 2)
    halo_a, halo_b = pl.pallas_call(
        lambda *refs: pack_body(band, slots, *refs),
        out_shape=[jax.ShapeDtypeStruct((BELOW, LANES * (slots + 2)), f32)] * 2,
        in_specs=[sm] + [vm] * 4,
        out_specs=[vm] * 2,
        name="pack",
    )(where, got_a, got_b, halo_a, halo_b)
    halo_a = paired(halo_a, "row", 0, False)
    halo_b = paired(halo_b, "row", 1, False)
    groups = -(-slots // 4) * 4
    out = pl.pallas_call(
        lambda *refs: main_body(dets, *refs),
        out_shape=jax.ShapeDtypeStruct((slots, band, LANES), f32),
        in_specs=[sm] * 2 + [vm] * 8,
        out_specs=vm,
        scratch_shapes=[
            pltpu.VMEM((rows + band, LANES), f32),
            pltpu.VMEM((band, LANES), f32),
            pltpu.SMEM((SPAN, 8, LANES), f32),
            pltpu.SemaphoreType.DMA((SPAN,)),
            pltpu.VMEM(((LANES + 8) * slots + 8, LANES), f32),
            pltpu.VMEM(((EDGE + 8) * (SPAN - 1) + 8, LANES), f32),
            pltpu.VMEM((LANES, LANES), f32),
            pltpu.VMEM((48, LANES), f32),
            pltpu.VMEM((40, LANES), f32),
            pltpu.VMEM((SPAN, 36 * 64, 2 * LANES), jnp.bfloat16),
            pltpu.VMEM((LANES * LONG + 72, LANES), f32),
            pltpu.VMEM((LANES * LONG + 72, LANES), f32),
            pltpu.VMEM((EDGE * groups, LANES), f32),
            pltpu.VMEM((EDGE * groups, LANES), f32),
            pltpu.VMEM((LANES, LANES), f32),
        ],
        name="subtract",
    )(where, tile_source, template[0], own, got_a, got_b, got_2, got_3, halo_a, halo_b)
    return out[None]


def solution(mesh):
    in_specs = (
        P("det", "row", None),
        P("det", None, "row", None),
        P(),
        P(None, "det", None),
        P(None, "det", None),
        P("det", None),
        P(),
        P("det", None),
        P("det"),
    )
    out_specs = P("det", None, "row", None)
    return jax.shard_map(body, mesh=mesh, in_specs=in_specs, out_specs=out_specs, check_vma=False)
```

```python
import jax
import jax.numpy as jnp
from jax import lax
from jax.experimental import pallas as pl
from jax.experimental.pallas import tpu as pltpu
from jax.sharding import PartitionSpec as P


SPAN = 4
LONG = 3
LANES = 128
ABOVE = 16
BELOW = 24
EDGE = 32
RIGHT = 24
LEFT = 16
FIRST = RIGHT * (SPAN - 1)
SMALL = pltpu.CompilerParams(vmem_limit_bytes=16 * 1024 * 1024)


def fdiv(value, divisor, bound):
    factor = 65536 // divisor + 1
    assert bound * (factor * divisor - 65536) < 65536
    return (value * factor) >> 16


def run_info(sources, row, slots, dets):
    columns = sources.shape[1]
    reach = []
    for c in range(columns):
        owner = fdiv(sources[row, c], slots, dets * slots)
        step = owner - row
        reach.append(jnp.where(step < 0, step + dets, step))
    starts, lengths = [], []
    for j in range(SPAN):
        starts.append(sum((x < j).astype(jnp.int32) for x in reach))
        lengths.append(sum((x == j).astype(jnp.int32) for x in reach))
    return starts, lengths


def wrap(value, count):
    return jnp.where(value < 0, value + count, value)


def lane_ids(rows):
    return lax.broadcasted_iota(jnp.int32, (rows, LANES), 1)


def row_ids(rows):
    return lax.broadcasted_iota(jnp.int32, (rows, LANES), 0)


def prep_body(dets, src, off, sw, valid, coef, back, sci, tmpl, basis,
              out_a, out_b, out_3, out_2, out_0, halo_a, halo_b, held, table, self_scal, kern):
    held[...] = tmpl[...]
    d = lax.axis_index("det")
    r = lax.axis_index("row")
    slots, band = tmpl.shape[0], tmpl.shape[1]
    columns = src.shape[1]
    even_d = lax.rem(d, 2) == 0
    even_r = lax.rem(r, 2) == 0
    starts, lengths = run_info(src, d, slots, dets)
    grow = row_ids(band) + r * band
    shade = jnp.broadcast_to(back[...], (band, LANES))

    tiles = []
    for j in range(SPAN):
        mine = []
        for k in range(LONG):
            c = jnp.minimum(starts[j] + k, columns - 1)
            limit = jnp.where(k < lengths[j], valid[0, c], 0)
            block = sci[:, pl.ds(pl.multiple_of(c * LANES, LANES), LANES)]
            mine.append(jnp.where(grow < limit, block - shade, 0.0))
        tiles.append(mine)

    tally = [jnp.int32(0) for _ in range(slots)]
    for j in range(SPAN):
        other = wrap(d - j, dets)
        st, ln = run_info(src, other, slots, dets)
        st, ln = st[j], ln[j]
        s0 = src[other, st] - d * slots
        table[4 * j] = st
        table[4 * j + 1] = ln
        table[4 * j + 2] = s0
        for s in range(slots):
            tally[s] = tally[s] + ((s0 <= s) & (s < s0 + ln)).astype(jnp.int32)
    for s in range(slots):
        table[4 * SPAN + s] = tally[s]
    for c in range(columns):
        self_scal[c, 0] = off[0, 0, c].astype(jnp.float32)
        self_scal[c, 1] = off[1, 0, c].astype(jnp.float32)
        self_scal[c, 2] = sw[0, 0, c]
        self_scal[c, 3] = sw[1, 0, c]
        self_scal[c, 4] = valid[0, c].astype(jnp.float32)

    width = basis.shape[1]
    total = coef[0, 0] * basis[0]
    for k in range(1, basis.shape[0]):
        total = total + coef[0, k] * basis[k]
    kern[...] = jnp.zeros_like(kern)
    kern[0:width, 0:width] = total
    flip = jnp.transpose(kern[...])
    packed = flip[0:8]
    for g in range(1, 4):
        packed = packed + pltpu.roll(flip[8 * g:8 * g + 8], EDGE * g, 1)

    lane8 = lane_ids(8)
    row8 = row_ids(8)
    params = jnp.zeros((8, LANES), jnp.float32)
    for c in range(columns):
        line = jnp.where(lane8 == 0, off[0, 0, c].astype(jnp.float32), 0.0)
        line = jnp.where(lane8 == 1, off[1, 0, c].astype(jnp.float32), line)
        line = jnp.where(lane8 == 2, sw[0, 0, c], line)
        line = jnp.where(lane8 == 3, sw[1, 0, c], line)
        line = jnp.where(lane8 == 4, valid[0, c].astype(jnp.float32), line)
        params = jnp.where(row8 == c, line, params)

    lane = lane_ids(band)
    left = jnp.zeros((band, LANES), jnp.float32)
    right = jnp.zeros((band, LANES), jnp.float32)
    for q in range(SPAN - 1):
        other = wrap(d - q, dets)
        st, ln = run_info(src, other, slots, dets)
        s = src[other, st[q] + ln[q] - 1] - d * slots
        at = FIRST + LEFT * q
        piece = pltpu.roll(tmpl[s], (at + LEFT) % LANES, 1)
        left = jnp.where((lane >= at) & (lane < at + LEFT), piece, left)
        other = wrap(d - q - 1, dets)
        st, ln = run_info(src, other, slots, dets)
        s = src[other, st[q + 1]] - d * slots
        piece = tmpl[s]
        if q:
            piece = pltpu.roll(piece, RIGHT * q, 1)
        right = jnp.where((lane >= RIGHT * q) & (lane < RIGHT * q + RIGHT), piece, right)

    def fill(ref, j):
        for k in range(LONG):
            ref[band * k:band * k + band] = tiles[j][k]
        ref[band * LONG:band * LONG + 8] = packed
        ref[band * LONG + 8:band * LONG + 16] = params

    fill(out_0, 0)
    fill(out_2, 2)
    fill(out_3, 3)

    def pair(plus, minus):
        fill(plus, 1)
        plus[band * LONG + 16:band * LONG + 16 + band] = left
        minus[0:band * LONG + 16] = jnp.zeros((band * LONG + 16, LANES), jnp.float32)
        minus[band * LONG + 16:band * LONG + 16 + band] = right

    @pl.when(even_d)
    def _():
        pair(out_a, out_b)

    @pl.when(jnp.logical_not(even_d))
    def _():
        pair(out_b, out_a)

    for s in range(slots):
        top = tmpl[s, 0:BELOW]
        bottom = tmpl[s, band - BELOW:band]
        halo_a[:, LANES * s:LANES * s + LANES] = jnp.where(even_r, bottom, top)
        halo_b[:, LANES * s:LANES * s + LANES] = jnp.where(even_r, top, bottom)


def pack_body(band, slots, got_a, got_b, in_a, halo_a, halo_s, strip):
    halo_a[:, 0:LANES * slots] = in_a[...]
    even_d = lax.rem(lax.axis_index("det"), 2) == 0
    even_r = lax.rem(lax.axis_index("row"), 2) == 0
    base = got_a.shape[0] - band
    from_a = got_a[base:base + band]
    from_b = got_b[base:base + band]
    left = jnp.where(even_d, from_b, from_a)
    right = jnp.where(even_d, from_a, from_b)
    both = jnp.where(lane_ids(band) < FIRST, right, left)
    strip[...] = both
    top = both[0:BELOW]
    bottom = both[band - BELOW:band]
    halo_a[:, LANES * slots:LANES * slots + LANES] = jnp.where(even_r, bottom, top)
    halo_s[...] = jnp.where(even_r, top, bottom)


def build_body(band, first, *refs):
    even_d = lax.rem(lax.axis_index("det"), 2) == 0
    at = band * LONG
    copies = []
    if first:
        own, got_a, got_b, vec_0, vec_1, kpad, rho = refs
        packs = [own[at:at + 8], jnp.where(even_d, got_b[at:at + 8], got_a[at:at + 8])]
    else:
        one, two, vec_0, vec_1, scal, kpad, rho, sem = refs
        packs = [one[at:at + 8], two[at:at + 8]]
        for i, ref in enumerate((one, two)):
            copies.append(pltpu.make_async_copy(ref.at[pl.ds(at + 8, 8), :], scal.at[i], sem.at[i]))
            copies[-1].start()
    lane = lane_ids(8)
    kpad[...] = jnp.zeros_like(kpad)
    back = (EDGE - lane // 4) % EDGE
    keep = (lane_ids(EDGE) // 4) <= row_ids(EDGE)
    for i, pk in enumerate(packs):
        vec = (vec_0, vec_1)[i]
        for g in range(4):
            kpad[8 + 8 * g:16 + 8 * g] = jnp.take_along_axis(pk, back + EDGE * g, axis=1)
        line = jnp.zeros((40, LANES), jnp.float32)
        dx = lane_ids(40) % 4
        for k in range(4):
            line = jnp.where(dx == k, kpad[8 - k:48 - k], line)
        rho[...] = line
        for u in range(36):
            one = jnp.broadcast_to(rho[u:u + 1], (EDGE, LANES))
            one = pltpu.roll(one, 0, 1, stride=4, stride_axis=0)
            high = one.astype(jnp.bfloat16).astype(jnp.float32)
            low = one - high
            at = 64 * u
            vec[at:at + EDGE, 0:LANES] = jnp.where(keep, high, 0.0).astype(jnp.bfloat16)
            vec[at + EDGE:at + 64, 0:LANES] = jnp.where(keep, 0.0, high).astype(jnp.bfloat16)
            vec[at:at + EDGE, LANES:2 * LANES] = jnp.where(keep, low, 0.0).astype(jnp.bfloat16)
            vec[at + EDGE:at + 64, LANES:2 * LANES] = jnp.where(keep, 0.0, low).astype(jnp.bfloat16)
    for c in copies:
        c.wait()


def read(scals, j, c, p):
    return scals[j % 2][c, p] if j < 2 else scals[j - 2, c, p]


def warp(r, band, scals, j, c, ref, at, count, ws, dst):
    ro = read(scals, j, c, 0).astype(jnp.int32)
    co = read(scals, j, c, 1).astype(jnp.int32)
    rw = read(scals, j, c, 2)
    cw = read(scals, j, c, 3)
    one = ref[pl.ds(at + co, count), :]
    two = ref[pl.ds(at + co + 1, count), :]
    mix = (1.0 - cw) * one + cw * two
    upper = pltpu.roll(mix, LANES - 1 - ro, 1)
    lower = pltpu.roll(mix, LANES - 2 - ro, 1)
    both = (1.0 - rw) * upper + rw * lower
    ids = lane_ids(count)
    grow = ids + (r * band - (ABOVE - 1))
    ok = (ids < 64) & (grow >= 0) & (grow < LANES)
    ws[pl.ds(dst, count), :] = jnp.where(ok, both, 0.0)


def conv(wt, vec, rows):
    total = jnp.zeros((2 * rows, 2 * LANES), jnp.float32)
    for t in range(9):
        one = wt[pl.ds(9 + 4 * t, rows, stride=4), :]
        two = wt[pl.ds(11 + 4 * t, rows, stride=4), :]
        lhs = jnp.concatenate([one, two], axis=1)
        high = lhs.astype(jnp.bfloat16)
        low = (lhs - high.astype(jnp.float32)).astype(jnp.bfloat16)
        total = total + jnp.dot(
            jnp.concatenate([high, low], axis=0), vec[256 * t:256 * t + 256],
            preferred_element_type=jnp.float32)
    res = total[0:rows] + total[rows:2 * rows]
    return res[:, 0:LANES] + res[:, LANES:2 * LANES]


def runs(pair, r, band, table, scals, tiles, lefts, rights, vecs, images, bufs, acc, sacc):
    tpad = LANES + 8
    spad = LEFT + 8
    where = {}
    for j in pair:
        ws, _ = bufs[j - pair[0]]
        st = table[4 * j]
        ln = table[4 * j + 1]
        where[j] = (st, ln, table[4 * j + 2])
        ws[...] = jnp.zeros_like(ws)
        if j > 0:
            warp(r, band, scals, j, st - 1, lefts, spad * (j - 1), LEFT, ws, 8)
        if j < SPAN - 1:
            end = pl.multiple_of(24 + LANES * ln, 8)
            warp(r, band, scals, j, st + ln, rights, RIGHT * j, 16, ws, end)

    def finish(counts):
        for j, count in zip(pair, counts):
            ws, wt = bufs[j - pair[0]]
            st, ln, s0 = where[j]
            for k in range(count):
                warp(r, band, scals, j, st + k, tiles, (s0 + k) * tpad, LANES, ws, 24 + LANES * k)
        for j, count in zip(pair, counts):
            ws, wt = bufs[j - pair[0]]
            n = LANES * count + 40
            wt[pl.ds(8, n), :] = ws[pl.ds(8, n), :] + pltpu.roll(ws[pl.ds(9, n), :], 64, 1)
        done = [conv(bufs[j - pair[0]][1], vecs[j - pair[0]], EDGE * count) for j, count in zip(pair, counts)]
        ids = lane_ids(EDGE) // 4 + r * band
        for j, count, res in zip(pair, counts, done):
            st, ln, s0 = where[j]
            for k in range(count):
                limit = read(scals, j, st + k, 4).astype(jnp.int32)
                piece = jnp.where(ids < limit, res[EDGE * k:EDGE * k + EDGE], 0.0)
                at = pl.multiple_of((s0 + k) * EDGE, EDGE)
                acc[pl.ds(at, EDGE), :] += piece
                sacc[pl.ds(at, EDGE), :] += images[j - pair[0]][band * k:band * k + band]

    one = [where[j][1] == 1 for j in pair]
    for a in (True, False):
        for b in (True, False):
            hit = (one[0] if a else jnp.logical_not(one[0])) & (one[1] if b else jnp.logical_not(one[1]))

            @pl.when(hit)
            def _(a=a, b=b):
                finish((1 if a else LONG, 1 if b else LONG))


def main_a(table, mine, tmpl, own, got_a, got_b, strip, halo_a, halo_t, halo_s, vec_0, vec_1,
           tiles, lefts, rights, acc, sacc,
           plus, scal, sem, ws0, wt0, ws1, wt1):
    d = lax.axis_index("det")
    r = lax.axis_index("row")
    slots, band = tmpl.shape[0], tmpl.shape[1]
    even_d = lax.rem(d, 2) == 0
    even_r = lax.rem(r, 2) == 0
    last = lax.axis_size("row") - 1
    tpad = LANES + 8
    spad = LEFT + 8
    plus[...] = jnp.where(even_d, got_b[0:plus.shape[0]], got_a[0:plus.shape[0]])
    copy = pltpu.make_async_copy(plus.at[pl.ds(band * LONG + 8, 8), :], scal, sem.at[0])
    copy.start()

    def stacked(middle, s):
        near_part = halo_a[:, LANES * s:LANES * s + LANES]
        far_part = halo_t[:, LANES * s:LANES * s + LANES] if s < slots else halo_s[...]
        up = jnp.where(even_r, far_part, near_part)[BELOW - ABOVE:BELOW]
        down = jnp.where(even_r, near_part, far_part)
        up = jnp.where(r == 0, 0.0, up)
        down = jnp.where(r == last, 0.0, down)
        return jnp.transpose(jnp.concatenate([up, middle, down], axis=0))

    tall = ABOVE + band + BELOW
    for s in range(slots):
        t = stacked(tmpl[s], s)
        tiles[tpad * s:tpad * s + LANES, 0:tall] = t
        tiles[tpad * s + LANES:tpad * s + tpad, 0:tall] = jnp.broadcast_to(t[LANES - 1:LANES], (8, tall))
    t = stacked(strip[...], slots)
    rights[:, 0:tall] = t
    for q in range(SPAN - 1):
        at = FIRST + LEFT * q
        lefts[spad * q:spad * q + LEFT, 0:tall] = t[at:at + LEFT]
        lefts[spad * q + LEFT:spad * q + spad, 0:tall] = jnp.broadcast_to(t[at + LEFT - 1:at + LEFT], (8, tall))

    acc[...] = jnp.zeros_like(acc)
    sacc[...] = jnp.zeros_like(sacc)
    copy.wait()
    runs((0, 1), r, band, table, (mine, scal), tiles, lefts, rights, (vec_0, vec_1), (own, plus),
         ((ws0, wt0), (ws1, wt1)), acc, sacc)


def main_b(table, scal_b, got_2, got_3, vec_2, vec_3, tiles, lefts, rights, acc_in, sacc_in, out,
           acc, sacc, tr, ws0, wt0, ws1, wt1):
    r = lax.axis_index("row")
    slots, band = out.shape[0], out.shape[1]
    acc[...] = acc_in[...]
    sacc[...] = sacc_in[...]
    runs((2, 3), r, band, table, scal_b, tiles, lefts, rights, (vec_2, vec_3), (got_2, got_3),
         ((ws0, wt0), (ws1, wt1)), acc, sacc)
    for g in range(0, slots, 4):
        tr[...] = jnp.transpose(acc[EDGE * g:EDGE * g + LANES])
        planes = [tr[pl.ds(k, EDGE, stride=4), :] for k in range(4)]
        ids = lane_ids(EDGE)
        for s in range(g, min(g + 4, slots)):
            pick = ids // 4 + EDGE * (s - g)
            image = jnp.zeros((EDGE, LANES), jnp.float32)
            for k in range(4):
                image = jnp.where(ids % 4 == k, jnp.take_along_axis(planes[k], pick, axis=1), image)
            scale = jnp.float32(1.0)
            for n in range(2, SPAN + 1):
                scale = jnp.where(table[4 * SPAN + s] == n, jnp.float32(1.0 / n), scale)
            out[s] = (sacc[EDGE * s:EDGE * s + EDGE] - image) * scale


def shifted(value, axis, steps):
    count = lax.axis_size(axis)
    return lax.ppermute(value, axis, [(i, (i + steps) % count) for i in range(count)])


def paired(value, axis, first, ring):
    count = lax.axis_size(axis)
    pairs = []
    for i in range(first, count if ring else count - 1, 2):
        k = (i + 1) % count
        pairs += [(i, k), (k, i)]
    left = set(range(count)) - {a for a, _ in pairs}
    pairs += [(i, i) for i in sorted(left)]
    return lax.ppermute(value, axis, pairs)


def body(science, template, tile_source, offsets, shift_weights, valid_rows, basis_kernels,
         coefficients, background):
    f32 = jnp.float32
    dets = lax.axis_size("det")
    assert dets % 2 == 0 and dets >= SPAN
    slots, band, tile = template.shape[1:]
    assert tile == LANES and band == EDGE
    vm = pl.BlockSpec(memory_space=pltpu.VMEM)
    sm = pl.BlockSpec(memory_space=pltpu.SMEM)
    near = lambda x: pltpu.with_memory_space_constraint(x, pltpu.VMEM)
    rows = band * LONG + 16
    shapes = [(rows + band, LANES)] * 2 + [(rows, LANES)] * 3 + [(BELOW, LANES * slots)] * 2
    shapes += [(slots, band, LANES)]
    out_a, out_b, out_3, out_2, own, halo_a, halo_b, held, table, mine = pl.pallas_call(
        lambda *refs: prep_body(dets, *refs),
        out_shape=[pltpu.VMEM(s, f32) for s in shapes] + [pltpu.SMEM((32,), jnp.int32), pltpu.SMEM((8, LANES), f32)],
        in_specs=[sm] * 5 + [vm] * 4,
        out_specs=[vm] * len(shapes) + [sm] * 2,
        scratch_shapes=[pltpu.VMEM((LANES, LANES), f32)],
        name="prep",
    )(tile_source, offsets, shift_weights, valid_rows, coefficients, background[None],
      science[0], template[0], basis_kernels)
    got_a = near(paired(out_a, "det", 0, False))
    got_b = near(paired(out_b, "det", 1, True))
    got_3 = near(shifted(out_3, "det", 3))
    got_2 = near(shifted(out_2, "det", 2))
    halo_t = near(paired(halo_b, "row", 1, True))
    halo_a, halo_s, strip = pl.pallas_call(
        lambda *refs: pack_body(band, slots, *refs),
        out_shape=[
            pltpu.VMEM((BELOW, LANES * (slots + 1)), f32),
            pltpu.VMEM((BELOW, LANES), f32),
            pltpu.VMEM((band, LANES), f32),
        ],
        in_specs=[vm] * 3,
        out_specs=[vm] * 3,
        name="pack",
    )(got_a, got_b, near(halo_a))
    halo_a = near(paired(halo_a, "row", 0, False))
    halo_s = near(paired(halo_s, "row", 1, True))
    own = near(own)
    size = (36 * 64, 2 * LANES)
    made = [pltpu.VMEM(size, jnp.bfloat16)] * 2
    work = [pltpu.VMEM((48, LANES), f32), pltpu.VMEM((40, LANES), f32)]
    close = lambda x: pltpu.with_memory_space_constraint(x, pltpu.SMEM)
    vec_0, vec_1 = pl.pallas_call(
        lambda *refs: build_body(band, True, *refs),
        out_shape=made,
        in_specs=[vm] * 3,
        out_specs=[vm] * 2,
        scratch_shapes=work,
        compiler_params=SMALL,
        name="build0",
    )(own, got_a, got_b)
    vec_2, vec_3, scal_b = pl.pallas_call(
        lambda *refs: build_body(band, False, *refs),
        out_shape=made + [pltpu.SMEM((2, 8, LANES), f32)],
        in_specs=[vm] * 2,
        out_specs=[vm, vm, sm],
        scratch_shapes=work + [pltpu.SemaphoreType.DMA((2,))],
        compiler_params=SMALL,
        name="build1",
    )(got_2, got_3)
    groups = -(-slots // 4) * 4
    flats = [
        pltpu.VMEM(((LANES + 8) * slots + 8, LANES), f32),
        pltpu.VMEM(((LEFT + 8) * (SPAN - 1), LANES), f32),
        pltpu.VMEM((LANES, LANES), f32),
        pltpu.VMEM((EDGE * groups, LANES), f32),
        pltpu.VMEM((EDGE * groups, LANES), f32),
    ]
    wide = [pltpu.VMEM((LANES * LONG + 72, LANES), f32)] * 4
    flat = pl.pallas_call(
        main_a,
        out_shape=flats,
        in_specs=[sm] * 2 + [vm] * 10,
        out_specs=[vm] * 5,
        scratch_shapes=[
            pltpu.VMEM((rows, LANES), f32),
            pltpu.SMEM((8, LANES), f32),
            pltpu.SemaphoreType.DMA((1,)),
        ] + wide,
        compiler_params=SMALL,
        name="main0",
    )(close(table), close(mine), near(held), own, got_a, got_b, near(strip),
      halo_a, halo_t, halo_s, near(vec_0), near(vec_1))
    out = pl.pallas_call(
        main_b,
        out_shape=jax.ShapeDtypeStruct((slots, band, LANES), f32),
        in_specs=[sm] * 2 + [vm] * 9,
        out_specs=vm,
        scratch_shapes=flats[3:] + [pltpu.VMEM((LANES, LANES), f32)] + wide,
        compiler_params=SMALL,
        name="main1",
    )(close(table), close(scal_b), got_2, got_3, near(vec_2), near(vec_3),
      *[near(x) for x in flat])
    return out[None]


def solution(mesh):
    in_specs = (
        P("det", "row", None),
        P("det", None, "row", None),
        P(),
        P(None, "det", None),
        P(None, "det", None),
        P("det", None),
        P(),
        P("det", None),
        P("det"),
    )
    out_specs = P("det", None, "row", None)

    return jax.shard_map(body, mesh=mesh, in_specs=in_specs, out_specs=out_specs, check_vma=False)
```

```python
import jax
import jax.numpy as jnp
from jax import lax
from jax.experimental import pallas as pl
from jax.experimental.pallas import tpu as pltpu
from jax.sharding import PartitionSpec as P


SPAN = 4
LONG = 3
LANES = 128
ABOVE = 16
BELOW = 24
EDGE = 32
RIGHT = 24
LEFT = 16
FIRST = RIGHT * (SPAN - 1)
SMALL = pltpu.CompilerParams(vmem_limit_bytes=16 * 1024 * 1024)


def wrap(value, count):
    return jnp.where(value < 0, value + count, value)


def run_info(sources, row, slots, dets):
    far = jnp.int32(SPAN - 1)
    for j in range(SPAN - 2, -1, -1):
        owner = row + j
        first = jnp.where(owner >= dets, owner - dets, owner) * slots
        value = sources[row, j + 1]
        far = jnp.where((value >= first) & (value < first + slots), j, far)
    extra = LONG - 1
    starts = [j + extra * (far < j).astype(jnp.int32) for j in range(SPAN)]
    lengths = [1 + extra * (far == j).astype(jnp.int32) for j in range(SPAN)]
    return starts, lengths


def lane_ids(rows):
    return lax.broadcasted_iota(jnp.int32, (rows, LANES), 1)


def row_ids(rows):
    return lax.broadcasted_iota(jnp.int32, (rows, LANES), 0)


def prep_body(dets, src, off, sw, valid, coef, back, sci, tmpl, basis,
              out_a, out_b, out_3, out_2, out_0, halo_a, halo_b, held, table, self_scal, kern):
    held[...] = tmpl[...]
    d = lax.axis_index("det")
    r = lax.axis_index("row")
    slots, band = tmpl.shape[0], tmpl.shape[1]
    columns = src.shape[1]
    even_d = lax.rem(d, 2) == 0
    even_r = lax.rem(r, 2) == 0
    assert columns == SPAN + LONG - 1
    others = [wrap(d - q, dets) for q in range(SPAN)]
    infos = [run_info(src, other, slots, dets) for other in others]
    starts, lengths = infos[0]
    grow = row_ids(band) + r * band
    shade = jnp.broadcast_to(back[...], (band, LANES))

    tiles = []
    for j in range(SPAN):
        mine = []
        for k in range(LONG):
            c = jnp.minimum(starts[j] + k, columns - 1)
            limit = jnp.where(k < lengths[j], valid[0, c], 0)
            block = sci[:, pl.ds(pl.multiple_of(c * LANES, LANES), LANES)]
            mine.append(jnp.where(grow < limit, block - shade, 0.0))
        tiles.append(mine)

    tally = [jnp.int32(0) for _ in range(slots)]
    for j in range(SPAN):
        st, ln = infos[j][0][j], infos[j][1][j]
        s0 = src[others[j], st] - d * slots
        table[4 * j] = st
        table[4 * j + 1] = ln
        table[4 * j + 2] = s0
        for s in range(slots):
            tally[s] = tally[s] + ((s0 <= s) & (s < s0 + ln)).astype(jnp.int32)
    for s in range(slots):
        table[4 * SPAN + s] = tally[s]
    for c in range(columns):
        self_scal[c, 0] = off[0, 0, c].astype(jnp.float32)
        self_scal[c, 1] = off[1, 0, c].astype(jnp.float32)
        self_scal[c, 2] = sw[0, 0, c]
        self_scal[c, 3] = sw[1, 0, c]
        self_scal[c, 4] = valid[0, c].astype(jnp.float32)

    width = basis.shape[1]
    total = coef[0, 0] * basis[0]
    for k in range(1, basis.shape[0]):
        total = total + coef[0, k] * basis[k]
    kern[...] = jnp.zeros_like(kern)
    kern[0:width, 0:width] = total
    flip = jnp.transpose(kern[...])
    packed = flip[0:8]
    for g in range(1, 4):
        packed = packed + pltpu.roll(flip[8 * g:8 * g + 8], EDGE * g, 1)

    lane8 = lane_ids(8)
    row8 = row_ids(8)
    params = jnp.zeros((8, LANES), jnp.float32)
    for c in range(columns):
        line = jnp.where(lane8 == 0, off[0, 0, c].astype(jnp.float32), 0.0)
        line = jnp.where(lane8 == 1, off[1, 0, c].astype(jnp.float32), line)
        line = jnp.where(lane8 == 2, sw[0, 0, c], line)
        line = jnp.where(lane8 == 3, sw[1, 0, c], line)
        line = jnp.where(lane8 == 4, valid[0, c].astype(jnp.float32), line)
        params = jnp.where(row8 == c, line, params)

    lane = lane_ids(band)
    left = jnp.zeros((band, LANES), jnp.float32)
    right = jnp.zeros((band, LANES), jnp.float32)
    for q in range(SPAN - 1):
        st, ln = infos[q]
        s = src[others[q], st[q] + ln[q] - 1] - d * slots
        at = FIRST + LEFT * q
        piece = pltpu.roll(tmpl[s], (at + LEFT) % LANES, 1)
        left = jnp.where((lane >= at) & (lane < at + LEFT), piece, left)
        s = src[others[q + 1], infos[q + 1][0][q + 1]] - d * slots
        piece = tmpl[s]
        if q:
            piece = pltpu.roll(piece, RIGHT * q, 1)
        right = jnp.where((lane >= RIGHT * q) & (lane < RIGHT * q + RIGHT), piece, right)

    def fill(ref, j):
        for k in range(LONG):
            ref[band * k:band * k + band] = tiles[j][k]
        ref[band * LONG:band * LONG + 8] = packed
        ref[band * LONG + 8:band * LONG + 16] = params

    fill(out_0, 0)
    fill(out_2, 2)
    fill(out_3, 3)

    def pair(plus, minus):
        fill(plus, 1)
        plus[band * LONG + 16:band * LONG + 16 + band] = left
        minus[0:band * LONG + 16] = jnp.zeros((band * LONG + 16, LANES), jnp.float32)
        minus[band * LONG + 16:band * LONG + 16 + band] = right

    @pl.when(even_d)
    def _():
        pair(out_a, out_b)

    @pl.when(jnp.logical_not(even_d))
    def _():
        pair(out_b, out_a)

    for s in range(slots):
        top = tmpl[s, 0:BELOW]
        bottom = tmpl[s, band - BELOW:band]
        halo_a[:, LANES * s:LANES * s + LANES] = jnp.where(even_r, bottom, top)
        halo_b[:, LANES * s:LANES * s + LANES] = jnp.where(even_r, top, bottom)


def pack_body(band, slots, got_a, got_b, in_a, halo_a, halo_s, strip):
    halo_a[:, 0:LANES * slots] = in_a[...]
    even_d = lax.rem(lax.axis_index("det"), 2) == 0
    even_r = lax.rem(lax.axis_index("row"), 2) == 0
    base = got_a.shape[0] - band
    from_a = got_a[base:base + band]
    from_b = got_b[base:base + band]
    left = jnp.where(even_d, from_b, from_a)
    right = jnp.where(even_d, from_a, from_b)
    both = jnp.where(lane_ids(band) < FIRST, right, left)
    strip[...] = both
    top = both[0:BELOW]
    bottom = both[band - BELOW:band]
    halo_a[:, LANES * slots:LANES * slots + LANES] = jnp.where(even_r, bottom, top)
    halo_s[...] = jnp.where(even_r, top, bottom)


def build_body(band, columns, first, *refs):
    even_d = lax.rem(lax.axis_index("det"), 2) == 0
    at = band * LONG
    if first:
        own, got_a, got_b, vec_0, vec_1, scal, kpad, rho = refs
        packs = [own[at:at + 8], jnp.where(even_d, got_b[at:at + 8], got_a[at:at + 8])]
        block = jnp.where(even_d, got_b[at + 8:at + 16], got_a[at + 8:at + 16])
        vecs = [vec_0, vec_1]
    else:
        one, vec_0, scal, kpad, rho = refs
        packs = [one[at:at + 8]]
        block = one[at + 8:at + 16]
        vecs = [vec_0]
    for c in range(columns):
        for p in range(5):
            scal[c, p] = block[c, p]
    lane = lane_ids(8)
    kpad[...] = jnp.zeros_like(kpad)
    back = (EDGE - lane // 4) % EDGE
    keep = (lane_ids(EDGE) // 4) <= row_ids(EDGE)
    for i, pk in enumerate(packs):
        vec = vecs[i]
        for g in range(4):
            kpad[8 + 8 * g:16 + 8 * g] = jnp.take_along_axis(pk, back + EDGE * g, axis=1)
        line = jnp.zeros((40, LANES), jnp.float32)
        dx = lane_ids(40) % 4
        for k in range(4):
            line = jnp.where(dx == k, kpad[8 - k:48 - k], line)
        rho[...] = line
        for u in range(36):
            one = jnp.broadcast_to(rho[u:u + 1], (EDGE, LANES))
            one = pltpu.roll(one, 0, 1, stride=4, stride_axis=0)
            high = one.astype(jnp.bfloat16).astype(jnp.float32)
            low = one - high
            at = 64 * u
            vec[at:at + EDGE, 0:LANES] = jnp.where(keep, high, 0.0).astype(jnp.bfloat16)
            vec[at + EDGE:at + 64, 0:LANES] = jnp.where(keep, 0.0, high).astype(jnp.bfloat16)
            vec[at:at + EDGE, LANES:2 * LANES] = jnp.where(keep, low, 0.0).astype(jnp.bfloat16)
            vec[at + EDGE:at + 64, LANES:2 * LANES] = jnp.where(keep, 0.0, low).astype(jnp.bfloat16)


def read(scals, j, c, p):
    return scals[j][c, p]


def warp(r, band, scals, j, c, ref, at, count, ws, dst):
    ro = read(scals, j, c, 0).astype(jnp.int32)
    co = read(scals, j, c, 1).astype(jnp.int32)
    rw = read(scals, j, c, 2)
    cw = read(scals, j, c, 3)
    one = ref[pl.ds(at + co, count), :]
    two = ref[pl.ds(at + co + 1, count), :]
    mix = (1.0 - cw) * one + cw * two
    upper = pltpu.roll(mix, LANES - 1 - ro, 1)
    lower = pltpu.roll(mix, LANES - 2 - ro, 1)
    both = (1.0 - rw) * upper + rw * lower
    ids = lane_ids(count)
    grow = ids + (r * band - (ABOVE - 1))
    ok = (ids < 64) & (grow >= 0) & (grow < LANES)
    ws[pl.ds(dst, count), :] = jnp.where(ok, both, 0.0)


def conv(wt, vec, rows):
    total = jnp.zeros((2 * rows, 2 * LANES), jnp.float32)
    for t in range(9):
        one = wt[pl.ds(9 + 4 * t, rows, stride=4), :]
        two = wt[pl.ds(11 + 4 * t, rows, stride=4), :]
        lhs = jnp.concatenate([one, two], axis=1)
        high = lhs.astype(jnp.bfloat16)
        low = (lhs - high.astype(jnp.float32)).astype(jnp.bfloat16)
        total = total + jnp.dot(
            jnp.concatenate([high, low], axis=0), vec[256 * t:256 * t + 256],
            preferred_element_type=jnp.float32)
    res = total[0:rows] + total[rows:2 * rows]
    return res[:, 0:LANES] + res[:, LANES:2 * LANES]


def edges(j, r, band, table, scals, lefts, rights, ws):
    st = table[4 * j]
    ln = table[4 * j + 1]
    end = pl.multiple_of(24 + LANES * ln, 8)
    blank = jnp.zeros((16, LANES), jnp.float32)
    if j > 0:
        warp(r, band, scals, j, st - 1, lefts, (LEFT + 8) * (j - 1), LEFT, ws, 8)
    else:
        ws[8:24] = blank
    ws[pl.ds(end + 16, 16), :] = blank
    if j < SPAN - 1:
        warp(r, band, scals, j, st + ln, rights, RIGHT * j, 16, ws, end)
    else:
        ws[pl.ds(end, 16), :] = blank


def runs(pair, r, band, table, scals, tiles, vecs, images, bufs, acc, sacc):
    tpad = LANES + 8
    where = {j: (table[4 * j], table[4 * j + 1], table[4 * j + 2]) for j in pair}

    def finish(counts):
        for j, count in zip(pair, counts):
            ws, wt = bufs[j - pair[0]]
            st, ln, s0 = where[j]
            for k in range(count):
                warp(r, band, scals, j, st + k, tiles, (s0 + k) * tpad, LANES, ws, 24 + LANES * k)
        for j, count in zip(pair, counts):
            ws, wt = bufs[j - pair[0]]
            n = LANES * count + 32
            wt[pl.ds(8, n), :] = ws[pl.ds(8, n), :] + pltpu.roll(ws[pl.ds(9, n), :], 64, 1)
        done = [conv(bufs[j - pair[0]][1], vecs[j - pair[0]], EDGE * count) for j, count in zip(pair, counts)]
        ids = lane_ids(EDGE) // 4 + r * band
        for j, count, res in zip(pair, counts, done):
            st, ln, s0 = where[j]
            for k in range(count):
                limit = read(scals, j, st + k, 4).astype(jnp.int32)
                piece = jnp.where(ids < limit, res[EDGE * k:EDGE * k + EDGE], 0.0)
                at = pl.multiple_of((s0 + k) * EDGE, EDGE)
                acc[pl.ds(at, EDGE), :] += piece
                sacc[pl.ds(at, EDGE), :] += images[j - pair[0]][band * k:band * k + band]

    one = [where[j][1] == 1 for j in pair]
    for a in (True, False):
        for b in (True, False):
            hit = (one[0] if a else jnp.logical_not(one[0])) & (one[1] if b else jnp.logical_not(one[1]))

            @pl.when(hit)
            def _(a=a, b=b):
                finish((1 if a else LONG, 1 if b else LONG))


def main_body(table, scal_0, scal_1, scal_2, scal_3, tmpl, own, got_a, got_b, got_2, got_3, strip, halo_a, halo_t, halo_s,
              vec_0, vec_1, vec_2, vec_3, out,
              tiles, lefts, rights, acc, sacc, plus, tr, done, sem, *bufs):
    d = lax.axis_index("det")
    r = lax.axis_index("row")
    slots, band = tmpl.shape[0], tmpl.shape[1]
    even_d = lax.rem(d, 2) == 0
    even_r = lax.rem(r, 2) == 0
    last = lax.axis_size("row") - 1
    tpad = LANES + 8
    spad = LEFT + 8
    plus[...] = jnp.where(even_d, got_b[0:plus.shape[0]], got_a[0:plus.shape[0]])

    def stacked(middle, s):
        near_part = halo_a[:, LANES * s:LANES * s + LANES]
        far_part = halo_t[:, LANES * s:LANES * s + LANES] if s < slots else halo_s[...]
        up = jnp.where(even_r, far_part, near_part)[BELOW - ABOVE:BELOW]
        down = jnp.where(even_r, near_part, far_part)
        up = jnp.where(r == 0, 0.0, up)
        down = jnp.where(r == last, 0.0, down)
        return jnp.transpose(jnp.concatenate([up, middle, down], axis=0))

    tall = ABOVE + band + BELOW
    for s in range(slots):
        t = stacked(tmpl[s], s)
        tiles[tpad * s:tpad * s + LANES, 0:tall] = t
        tiles[tpad * s + LANES:tpad * s + tpad, 0:tall] = jnp.broadcast_to(t[LANES - 1:LANES], (8, tall))
    t = stacked(strip[...], slots)
    rights[:, 0:tall] = t
    for q in range(SPAN - 1):
        at = FIRST + LEFT * q
        lefts[spad * q:spad * q + LEFT, 0:tall] = t[at:at + LEFT]
        lefts[spad * q + LEFT:spad * q + spad, 0:tall] = jnp.broadcast_to(t[at + LEFT - 1:at + LEFT], (8, tall))

    acc[...] = jnp.zeros_like(acc)
    sacc[...] = jnp.zeros_like(sacc)
    scals = (scal_0, scal_1, scal_2, scal_3)
    for j in range(SPAN):
        edges(j, r, band, table, scals, lefts, rights, bufs[2 * j])
    vecs = (vec_0, vec_1, vec_2, vec_3)
    images = (own, plus, got_2, got_3)
    for a in range(0, SPAN, 2):
        span = [(bufs[2 * j], bufs[2 * j + 1]) for j in (a, a + 1)]
        runs((a, a + 1), r, band, table, scals, tiles, vecs[a:a + 2], images[a:a + 2], span, acc, sacc)
    copies = []
    for g in range(0, slots, 4):
        tr[...] = jnp.transpose(acc[EDGE * g:EDGE * g + LANES])
        planes = [tr[pl.ds(k, EDGE, stride=4), :] for k in range(4)]
        ids = lane_ids(EDGE)
        for s in range(g, min(g + 4, slots)):
            pick = ids // 4 + EDGE * (s - g)
            image = jnp.zeros((EDGE, LANES), jnp.float32)
            for k in range(4):
                image = jnp.where(ids % 4 == k, jnp.take_along_axis(planes[k], pick, axis=1), image)
            scale = jnp.float32(1.0)
            for n in range(2, SPAN + 1):
                scale = jnp.where(table[4 * SPAN + s] == n, jnp.float32(1.0 / n), scale)
            done[s] = (sacc[EDGE * s:EDGE * s + EDGE] - image) * scale
            copies.append(pltpu.make_async_copy(done.at[s], out.at[s], sem.at[s]))
            copies[-1].start()
    for c in copies:
        c.wait()


def shifted(value, axis, steps):
    count = lax.axis_size(axis)
    return lax.ppermute(value, axis, [(i, (i + steps) % count) for i in range(count)])


def paired(value, axis, first, ring):
    count = lax.axis_size(axis)
    pairs = []
    for i in range(first, count if ring else count - 1, 2):
        k = (i + 1) % count
        pairs += [(i, k), (k, i)]
    left = set(range(count)) - {a for a, _ in pairs}
    pairs += [(i, i) for i in sorted(left)]
    return lax.ppermute(value, axis, pairs)


def body(science, template, tile_source, offsets, shift_weights, valid_rows, basis_kernels,
         coefficients, background):
    f32 = jnp.float32
    dets = lax.axis_size("det")
    assert dets % 2 == 0 and dets >= SPAN
    slots, band, tile = template.shape[1:]
    assert tile == LANES and band == EDGE
    columns = science.shape[2] // tile
    vm = pl.BlockSpec(memory_space=pltpu.VMEM)
    sm = pl.BlockSpec(memory_space=pltpu.SMEM)
    near = lambda x: pltpu.with_memory_space_constraint(x, pltpu.VMEM)
    rows = band * LONG + 16
    shapes = [(rows + band, LANES)] * 2 + [(rows, LANES)] * 3 + [(BELOW, LANES * slots)] * 2
    shapes += [(slots, band, LANES)]
    out_a, out_b, out_3, out_2, own, halo_a, halo_b, held, table, mine = pl.pallas_call(
        lambda *refs: prep_body(dets, *refs),
        out_shape=[pltpu.VMEM(s, f32) for s in shapes] + [pltpu.SMEM((32,), jnp.int32), pltpu.SMEM((8, LANES), f32)],
        in_specs=[sm] * 5 + [vm] * 4,
        out_specs=[vm] * len(shapes) + [sm] * 2,
        scratch_shapes=[pltpu.VMEM((LANES, LANES), f32)],
        name="prep",
    )(tile_source, offsets, shift_weights, valid_rows, coefficients, background[None],
      science[0], template[0], basis_kernels)
    got_a = near(paired(out_a, "det", 0, False))
    got_b = near(paired(out_b, "det", 1, True))
    got_3 = near(shifted(out_3, "det", 3))
    got_2 = near(shifted(out_2, "det", 2))
    halo_t = near(paired(halo_b, "row", 1, True))
    halo_a, halo_s, strip = pl.pallas_call(
        lambda *refs: pack_body(band, slots, *refs),
        out_shape=[
            pltpu.VMEM((BELOW, LANES * (slots + 1)), f32),
            pltpu.VMEM((BELOW, LANES), f32),
            pltpu.VMEM((band, LANES), f32),
        ],
        in_specs=[vm] * 3,
        out_specs=[vm] * 3,
        name="pack",
    )(got_a, got_b, near(halo_a))
    halo_a = near(paired(halo_a, "row", 0, False))
    halo_s = near(paired(halo_s, "row", 1, True))
    own = near(own)
    size = (36 * 64, 2 * LANES)
    made = pltpu.VMEM(size, jnp.bfloat16)
    facts = pltpu.SMEM((8, LANES), f32)
    work = [pltpu.VMEM((48, LANES), f32), pltpu.VMEM((40, LANES), f32)]
    close = lambda x: pltpu.with_memory_space_constraint(x, pltpu.SMEM)
    vec_0, vec_1, scal_1 = pl.pallas_call(
        lambda *refs: build_body(band, columns, True, *refs),
        out_shape=[made, made, facts],
        in_specs=[vm] * 3,
        out_specs=[vm, vm, sm],
        scratch_shapes=work,
        compiler_params=SMALL,
        name="build0",
    )(own, got_a, got_b)
    late = pl.pallas_call(
        lambda *refs: build_body(band, columns, False, *refs),
        out_shape=[made, facts],
        in_specs=[vm],
        out_specs=[vm, sm],
        scratch_shapes=work,
        compiler_params=SMALL,
        name="build1",
    )
    vec_3, scal_3 = late(got_3)
    vec_2, scal_2 = late(got_2)
    groups = -(-slots // 4) * 4
    out = pl.pallas_call(
        main_body,
        out_shape=jax.ShapeDtypeStruct((slots, band, LANES), f32),
        in_specs=[sm] * 5 + [vm] * 14,
        out_specs=pl.BlockSpec(memory_space=pl.ANY),
        scratch_shapes=[
            pltpu.VMEM(((LANES + 8) * slots + 8, LANES), f32),
            pltpu.VMEM(((LEFT + 8) * (SPAN - 1), LANES), f32),
            pltpu.VMEM((LANES, LANES), f32),
            pltpu.VMEM((EDGE * groups, LANES), f32),
            pltpu.VMEM((EDGE * groups, LANES), f32),
            pltpu.VMEM((rows, LANES), f32),
            pltpu.VMEM((LANES, LANES), f32),
            pltpu.VMEM((slots, band, LANES), f32),
            pltpu.SemaphoreType.DMA((slots,)),
        ] + [pltpu.VMEM((LANES * LONG + 72, LANES), f32)] * (2 * SPAN),
        compiler_params=SMALL,
        name="subtract",
    )(close(table), close(mine), close(scal_1), close(scal_2), close(scal_3), near(held), own, got_a, got_b, got_2, got_3,
      near(strip), halo_a, halo_t, halo_s, near(vec_0), near(vec_1), near(vec_2), near(vec_3))
    return out[None]


def solution(mesh):
    in_specs = (
        P("det", "row", None),
        P("det", None, "row", None),
        P(),
        P(None, "det", None),
        P(None, "det", None),
        P("det", None),
        P(),
        P("det", None),
        P("det"),
    )
    out_specs = P("det", None, "row", None)

    return jax.shard_map(body, mesh=mesh, in_specs=in_specs, out_specs=out_specs, check_vma=False)
```

```python
import jax
import jax.numpy as jnp
from jax import lax
from jax.experimental import pallas as pl
from jax.experimental.pallas import tpu as pltpu
from jax.sharding import PartitionSpec as P


SPAN = 4
LONG = 3
LANES = 128
ABOVE = 16
BELOW = 24
EDGE = 32
RIGHT = 24
LEFT = 16
FIRST = RIGHT * (SPAN - 1)
SMALL = pltpu.CompilerParams(vmem_limit_bytes=16 * 1024 * 1024)
TIGHT = pltpu.CompilerParams(
    vmem_limit_bytes=16 * 1024 * 1024)


def wrap(value, count):
    return jnp.where(value < 0, value + count, value)


def run_info(sources, row, slots, dets):
    far = jnp.int32(SPAN - 1)
    for j in range(SPAN - 2, -1, -1):
        owner = row + j
        first = jnp.where(owner >= dets, owner - dets, owner) * slots
        value = sources[row, j + 1]
        far = jnp.where((value >= first) & (value < first + slots), j, far)
    extra = LONG - 1
    starts = [j + extra * (far < j).astype(jnp.int32) for j in range(SPAN)]
    lengths = [1 + extra * (far == j).astype(jnp.int32) for j in range(SPAN)]
    return starts, lengths


def lane_ids(rows):
    return lax.broadcasted_iota(jnp.int32, (rows, LANES), 1)


def row_ids(rows):
    return lax.broadcasted_iota(jnp.int32, (rows, LANES), 0)


def prep_body(dets, *refs):
    far = refs[0:9]
    out_a, out_b, out_3, out_2, out_0, halo_a, halo_b, held, table, facts = refs[9:19]
    here = refs[19:28]
    kern, sem = refs[28:30]
    copies = [pltpu.make_async_copy(x, y, sem.at[i]) for i, (x, y) in enumerate(zip(far, here))]
    for c in copies:
        c.start()
    src, off, sw, valid, coef, back, tmpl, sci, basis = here
    for c in copies[:6]:
        c.wait()
    d = lax.axis_index("det")
    r = lax.axis_index("row")
    slots, band = tmpl.shape[0], tmpl.shape[1]
    columns = src.shape[1]
    assert columns == SPAN + LONG - 1
    even_d = lax.rem(d, 2) == 0
    even_r = lax.rem(r, 2) == 0
    others = [wrap(d - q, dets) for q in range(SPAN)]
    infos = [run_info(src, other, slots, dets) for other in others]
    starts, lengths = infos[0]
    tally = [jnp.int32(0) for _ in range(slots)]
    for j in range(SPAN):
        st, ln = infos[j][0][j], infos[j][1][j]
        s0 = src[others[j], st] - d * slots
        table[4 * j] = st
        table[4 * j + 1] = ln
        table[4 * j + 2] = s0
        for s in range(slots):
            tally[s] = tally[s] + ((s0 <= s) & (s < s0 + ln)).astype(jnp.int32)
    for s in range(slots):
        table[4 * SPAN + s] = tally[s]
    lane8 = lane_ids(8)
    row8 = row_ids(8)
    params = jnp.zeros((8, LANES), jnp.float32)
    for c in range(columns):
        line = jnp.zeros((8, LANES), jnp.float32)
        fact = (off[0, 0, c].astype(jnp.float32), off[1, 0, c].astype(jnp.float32), sw[0, 0, c], sw[1, 0, c],
                valid[0, c].astype(jnp.float32))
        for i, value in enumerate(fact):
            facts[c, i] = value
            line = jnp.where(lane8 == i, value, line)
        params = jnp.where(row8 == c, line, params)
    lead = band * LONG
    for ref in (out_0, out_2, out_3, out_a, out_b):
        ref[lead + 8:lead + 16] = params

    copies[6].wait()
    held[...] = tmpl[...]
    lane = lane_ids(band)
    left = jnp.zeros((band, LANES), jnp.float32)
    right = jnp.zeros((band, LANES), jnp.float32)
    for q in range(SPAN - 1):
        st, ln = infos[q]
        s = src[others[q], st[q] + ln[q] - 1] - d * slots
        at = FIRST + LEFT * q
        piece = pltpu.roll(tmpl[s], (at + LEFT) % LANES, 1)
        left = jnp.where((lane >= at) & (lane < at + LEFT), piece, left)
        s = src[others[q + 1], infos[q + 1][0][q + 1]] - d * slots
        piece = tmpl[s]
        if q:
            piece = pltpu.roll(piece, RIGHT * q, 1)
        right = jnp.where((lane >= RIGHT * q) & (lane < RIGHT * q + RIGHT), piece, right)
    out_a[lead + 16:lead + 16 + band] = jnp.where(even_d, left, right)
    out_b[lead + 16:lead + 16 + band] = jnp.where(even_d, right, left)
    for s in range(slots):
        top = tmpl[s, 0:BELOW]
        bottom = tmpl[s, band - BELOW:band]
        halo_a[:, LANES * s:LANES * s + LANES] = jnp.where(even_r, bottom, top)
        halo_b[:, LANES * s:LANES * s + LANES] = jnp.where(even_r, top, bottom)

    copies[7].wait()
    grow = row_ids(band) + r * band
    for j, places in enumerate(((out_0,), (out_a, out_b), (out_2,), (out_3,))):
        for k in range(LONG):
            c = jnp.minimum(starts[j] + k, columns - 1)
            limit = jnp.where(k < lengths[j], valid[0, c], 0)
            block = sci[:, pl.ds(pl.multiple_of(c * LANES, LANES), LANES)]
            block = jnp.where(grow < limit, block - back[0, 0], 0.0)
            for ref in places:
                ref[band * k:band * k + band] = block

    width = basis.shape[1]
    kern[...] = jnp.zeros_like(kern)
    copies[8].wait()
    total = coef[0, 0] * basis[0]
    for k in range(1, basis.shape[0]):
        total = total + coef[0, k] * basis[k]
    kern[0:width, 0:width] = total
    flip = jnp.transpose(kern[...])
    packed = flip[0:8]
    for g in range(1, 4):
        packed = packed + pltpu.roll(flip[8 * g:8 * g + 8], EDGE * g, 1)
    for ref in (out_0, out_2, out_3, out_a, out_b):
        ref[lead:lead + 8] = packed


def pack_body(band, slots, got_a, got_b, in_a, halo_a, halo_s, strip):
    halo_a[:, 0:LANES * slots] = in_a[...]
    even_d = lax.rem(lax.axis_index("det"), 2) == 0
    even_r = lax.rem(lax.axis_index("row"), 2) == 0
    base = got_a.shape[0] - band
    from_a = got_a[base:base + band]
    from_b = got_b[base:base + band]
    left = jnp.where(even_d, from_b, from_a)
    right = jnp.where(even_d, from_a, from_b)
    both = jnp.where(lane_ids(band) < FIRST, right, left)
    strip[...] = both
    top = both[0:BELOW]
    bottom = both[band - BELOW:band]
    halo_a[:, LANES * slots:LANES * slots + LANES] = jnp.where(even_r, bottom, top)
    halo_s[...] = jnp.where(even_r, top, bottom)


def build_body(band, columns, first, *refs):
    even_d = lax.rem(lax.axis_index("det"), 2) == 0
    at = band * LONG
    if first:
        own, got_a, got_b, vec_0, vec_1, scal, kpad, rho = refs
        packs = [own[at:at + 8], jnp.where(even_d, got_b[at:at + 8], got_a[at:at + 8])]
        block = jnp.where(even_d, got_b[at + 8:at + 16], got_a[at + 8:at + 16])
        vecs = [vec_0, vec_1]
    else:
        one, vec_0, scal, kpad, rho = refs
        packs = [one[at:at + 8]]
        block = one[at + 8:at + 16]
        vecs = [vec_0]
    for c in range(columns):
        for p in range(5):
            scal[c, p] = block[c, p]
    lane = lane_ids(8)
    kpad[...] = jnp.zeros_like(kpad)
    back = (EDGE - lane // 4) % EDGE
    keep = (lane_ids(EDGE) // 4) <= row_ids(EDGE)
    lower = jnp.where(keep, 1.0, 0.0).astype(jnp.bfloat16)
    upper = jnp.where(keep, 0.0, 1.0).astype(jnp.bfloat16)
    for i, pk in enumerate(packs):
        vec = vecs[i]
        for g in range(4):
            kpad[8 + 8 * g:16 + 8 * g] = jnp.take_along_axis(pk, back + EDGE * g, axis=1)
        line = jnp.zeros((40, LANES), jnp.float32)
        dx = lane_ids(40) % 4
        for k in range(4):
            line = jnp.where(dx == k, kpad[8 - k:48 - k], line)
        rho[...] = line
        for u in range(36):
            one = jnp.broadcast_to(rho[u:u + 1], (EDGE, LANES))
            one = pltpu.roll(one, 0, 1, stride=4, stride_axis=0)
            high = one.astype(jnp.bfloat16)
            low = (one - high.astype(jnp.float32)).astype(jnp.bfloat16)
            at = 64 * u
            vec[at:at + EDGE, 0:LANES] = high * lower
            vec[at + EDGE:at + 64, 0:LANES] = high * upper
            vec[at:at + EDGE, LANES:2 * LANES] = low * lower
            vec[at + EDGE:at + 64, LANES:2 * LANES] = low * upper


def read(scals, j, c, p):
    return scals[j][c, p]


def warp(r, band, scals, j, c, ref, at, count, ws, dst):
    ro = read(scals, j, c, 0).astype(jnp.int32)
    co = read(scals, j, c, 1).astype(jnp.int32)
    rw = read(scals, j, c, 2)
    cw = read(scals, j, c, 3)
    one = ref[pl.ds(at + co, count), :]
    two = ref[pl.ds(at + co + 1, count), :]
    mix = (1.0 - cw) * one + cw * two
    upper = pltpu.roll(mix, LANES - 1 - ro, 1)
    lower = pltpu.roll(mix, LANES - 2 - ro, 1)
    both = (1.0 - rw) * upper + rw * lower
    ids = lane_ids(count)
    grow = ids + (r * band - (ABOVE - 1))
    ok = (ids < 64) & (grow >= 0) & (grow < LANES)
    ws[pl.ds(dst, count), :] = jnp.where(ok, both, 0.0)


def conv(wt, vec, rows):
    total = jnp.zeros((2 * rows, 2 * LANES), jnp.float32)
    for t in range(9):
        one = wt[pl.ds(9 + 4 * t, rows, stride=4), :]
        two = wt[pl.ds(11 + 4 * t, rows, stride=4), :]
        lhs = jnp.concatenate([one, two], axis=1)
        high = lhs.astype(jnp.bfloat16)
        low = (lhs - high.astype(jnp.float32)).astype(jnp.bfloat16)
        total = total + jnp.dot(
            jnp.concatenate([high, low], axis=0), vec[256 * t:256 * t + 256],
            preferred_element_type=jnp.float32)
    res = total[0:rows] + total[rows:2 * rows]
    return res[:, 0:LANES] + res[:, LANES:2 * LANES]


def edges(j, r, band, table, scals, lefts, rights, ws):
    st = table[4 * j]
    ln = table[4 * j + 1]
    end = pl.multiple_of(24 + LANES * ln, 8)
    blank = jnp.zeros((16, LANES), jnp.float32)
    if j > 0:
        warp(r, band, scals, j, st - 1, lefts, (LEFT + 8) * (j - 1), LEFT, ws, 8)
    else:
        ws[8:24] = blank
    ws[pl.ds(end + 16, 16), :] = blank
    if j < SPAN - 1:
        warp(r, band, scals, j, st + ln, rights, RIGHT * j, 16, ws, end)
    else:
        ws[pl.ds(end, 16), :] = blank


def runs(pair, r, band, table, scals, tiles, vecs, images, bufs, acc, sacc):
    tpad = LANES + 8
    where = {j: (table[4 * j], table[4 * j + 1], table[4 * j + 2]) for j in pair}

    def finish(counts):
        for j, count in zip(pair, counts):
            ws, wt = bufs[j - pair[0]]
            st, ln, s0 = where[j]
            for k in range(count):
                warp(r, band, scals, j, st + k, tiles, (s0 + k) * tpad, LANES, ws, 24 + LANES * k)
        for j, count in zip(pair, counts):
            ws, wt = bufs[j - pair[0]]
            n = LANES * count + 32
            wt[pl.ds(8, n), :] = ws[pl.ds(8, n), :] + pltpu.roll(ws[pl.ds(9, n), :], 64, 1)
        done = [conv(bufs[j - pair[0]][1], vecs[j - pair[0]], EDGE * count) for j, count in zip(pair, counts)]
        ids = lane_ids(EDGE) // 4 + r * band
        for j, count, res in zip(pair, counts, done):
            st, ln, s0 = where[j]
            for k in range(count):
                limit = read(scals, j, st + k, 4).astype(jnp.int32)
                piece = jnp.where(ids < limit, res[EDGE * k:EDGE * k + EDGE], 0.0)
                at = pl.multiple_of((s0 + k) * EDGE, EDGE)
                acc[pl.ds(at, EDGE), :] += piece
                sacc[pl.ds(at, EDGE), :] += images[j - pair[0]][band * k:band * k + band]

    one = [where[j][1] == 1 for j in pair]
    for a in (True, False):
        for b in (True, False):
            hit = (one[0] if a else jnp.logical_not(one[0])) & (one[1] if b else jnp.logical_not(one[1]))

            @pl.when(hit)
            def _(a=a, b=b):
                finish((1 if a else LONG, 1 if b else LONG))


def main_body(table, scal_0, scal_1, scal_2, scal_3, tmpl, own, got_a, got_b, got_2, got_3, strip, halo_a, halo_t, halo_s,
              vec_0, vec_1, vec_2, vec_3, out,
              tiles, lefts, rights, acc, sacc, plus, tr, done, sem, *bufs):
    d = lax.axis_index("det")
    r = lax.axis_index("row")
    slots, band = tmpl.shape[0], tmpl.shape[1]
    even_d = lax.rem(d, 2) == 0
    even_r = lax.rem(r, 2) == 0
    last = lax.axis_size("row") - 1
    tpad = LANES + 8
    spad = LEFT + 8
    plus[...] = jnp.where(even_d, got_b[0:plus.shape[0]], got_a[0:plus.shape[0]])

    def stacked(middle, s):
        near_part = halo_a[:, LANES * s:LANES * s + LANES]
        far_part = halo_t[:, LANES * s:LANES * s + LANES] if s < slots else halo_s[...]
        up = jnp.where(even_r, far_part, near_part)[BELOW - ABOVE:BELOW]
        down = jnp.where(even_r, near_part, far_part)
        up = jnp.where(r == 0, 0.0, up)
        down = jnp.where(r == last, 0.0, down)
        return jnp.transpose(jnp.concatenate([up, middle, down], axis=0))

    tall = ABOVE + band + BELOW
    for s in range(slots):
        t = stacked(tmpl[s], s)
        tiles[tpad * s:tpad * s + LANES, 0:tall] = t
        tiles[tpad * s + LANES:tpad * s + tpad, 0:tall] = jnp.broadcast_to(t[LANES - 1:LANES], (8, tall))
    t = stacked(strip[...], slots)
    rights[:, 0:tall] = t
    for q in range(SPAN - 1):
        at = FIRST + LEFT * q
        lefts[spad * q:spad * q + LEFT, 0:tall] = t[at:at + LEFT]
        lefts[spad * q + LEFT:spad * q + spad, 0:tall] = jnp.broadcast_to(t[at + LEFT - 1:at + LEFT], (8, tall))

    acc[...] = jnp.zeros_like(acc)
    sacc[...] = jnp.zeros_like(sacc)
    scals = (scal_0, scal_1, scal_2, scal_3)
    for j in range(SPAN):
        edges(j, r, band, table, scals, lefts, rights, bufs[2 * j])
    vecs = (vec_0, vec_1, vec_2, vec_3)
    images = (own, plus, got_2, got_3)
    for a in range(0, SPAN, 2):
        span = [(bufs[2 * j], bufs[2 * j + 1]) for j in (a, a + 1)]
        runs((a, a + 1), r, band, table, scals, tiles, vecs[a:a + 2], images[a:a + 2], span, acc, sacc)
    copies = []
    for g in range(0, slots, 4):
        tr[...] = jnp.transpose(acc[EDGE * g:EDGE * g + LANES])
        planes = [tr[pl.ds(k, EDGE, stride=4), :] for k in range(4)]
        ids = lane_ids(EDGE)
        for s in range(g, min(g + 4, slots)):
            pick = ids // 4 + EDGE * (s - g)
            image = jnp.zeros((EDGE, LANES), jnp.float32)
            for k in range(4):
                image = jnp.where(ids % 4 == k, jnp.take_along_axis(planes[k], pick, axis=1), image)
            scale = jnp.float32(1.0)
            for n in range(2, SPAN + 1):
                scale = jnp.where(table[4 * SPAN + s] == n, jnp.float32(1.0 / n), scale)
            done[s] = (sacc[EDGE * s:EDGE * s + EDGE] - image) * scale
            copies.append(pltpu.make_async_copy(done.at[s], out.at[s], sem.at[s]))
            copies[-1].start()
    for c in copies:
        c.wait()


def shifted(value, axis, steps):
    count = lax.axis_size(axis)
    return lax.ppermute(value, axis, [(i, (i + steps) % count) for i in range(count)])


def paired(value, axis, first, ring):
    count = lax.axis_size(axis)
    pairs = []
    for i in range(first, count if ring else count - 1, 2):
        k = (i + 1) % count
        pairs += [(i, k), (k, i)]
    left = set(range(count)) - {a for a, _ in pairs}
    pairs += [(i, i) for i in sorted(left)]
    return lax.ppermute(value, axis, pairs)


def body(science, template, tile_source, offsets, shift_weights, valid_rows, basis_kernels,
         coefficients, background):
    f32 = jnp.float32
    dets = lax.axis_size("det")
    assert dets % 2 == 0 and dets >= SPAN
    slots, band, tile = template.shape[1:]
    assert tile == LANES and band == EDGE
    columns = science.shape[2] // tile
    vm = pl.BlockSpec(memory_space=pltpu.VMEM)
    sm = pl.BlockSpec(memory_space=pltpu.SMEM)
    near = lambda x: pltpu.with_memory_space_constraint(x, pltpu.VMEM)
    rows = band * LONG + 16
    shapes = [(rows + band, LANES)] * 2 + [(rows, LANES)] * 3 + [(BELOW, LANES * slots)] * 2
    shapes += [(slots, band, LANES)]
    inputs = (tile_source, offsets, shift_weights, valid_rows, coefficients, background[None],
              template[0], science[0], basis_kernels)
    out_a, out_b, out_3, out_2, own, halo_a, halo_b, held, table, mine = pl.pallas_call(
        lambda *refs: prep_body(dets, *refs),
        out_shape=[pltpu.VMEM(s, f32) for s in shapes] + [pltpu.SMEM((32,), jnp.int32), pltpu.SMEM((8, LANES), f32)],
        in_specs=[pl.BlockSpec(memory_space=pl.ANY)] * 9,
        out_specs=[vm] * len(shapes) + [sm] * 2,
        scratch_shapes=[pltpu.SMEM(x.shape, x.dtype) for x in inputs[:6]]
        + [pltpu.VMEM(x.shape, x.dtype) for x in inputs[6:]]
        + [pltpu.VMEM((LANES, LANES), f32), pltpu.SemaphoreType.DMA((9,))],
        name="prep",
    )(*inputs)
    got_a = near(paired(out_a, "det", 0, False))
    got_b = near(paired(out_b, "det", 1, True))
    got_3 = near(shifted(out_3, "det", 3))
    got_2 = near(shifted(out_2, "det", 2))
    halo_t = near(paired(halo_b, "row", 1, True))
    halo_a, halo_s, strip = pl.pallas_call(
        lambda *refs: pack_body(band, slots, *refs),
        out_shape=[
            pltpu.VMEM((BELOW, LANES * (slots + 1)), f32),
            pltpu.VMEM((BELOW, LANES), f32),
            pltpu.VMEM((band, LANES), f32),
        ],
        in_specs=[vm] * 3,
        out_specs=[vm] * 3,
        name="pack",
    )(got_a, got_b, near(halo_a))
    halo_a = near(paired(halo_a, "row", 0, False))
    halo_s = near(paired(halo_s, "row", 1, True))
    own = near(own)
    size = (36 * 64, 2 * LANES)
    made = pltpu.VMEM(size, jnp.bfloat16)
    facts = pltpu.SMEM((8, LANES), f32)
    work = [pltpu.VMEM((48, LANES), f32), pltpu.VMEM((40, LANES), f32)]
    close = lambda x: pltpu.with_memory_space_constraint(x, pltpu.SMEM)
    vec_0, vec_1, scal_1 = pl.pallas_call(
        lambda *refs: build_body(band, columns, True, *refs),
        out_shape=[made, made, facts],
        in_specs=[vm] * 3,
        out_specs=[vm, vm, sm],
        scratch_shapes=work,
        compiler_params=SMALL,
        name="build0",
    )(own, got_a, got_b)
    late = pl.pallas_call(
        lambda *refs: build_body(band, columns, False, *refs),
        out_shape=[made, facts],
        in_specs=[vm],
        out_specs=[vm, sm],
        scratch_shapes=work,
        compiler_params=SMALL,
        name="build1",
    )
    vec_3, scal_3 = late(got_3)
    vec_2, scal_2 = late(got_2)
    groups = -(-slots // 4) * 4
    out = pl.pallas_call(
        main_body,
        out_shape=jax.ShapeDtypeStruct((slots, band, LANES), f32),
        in_specs=[sm] * 5 + [vm] * 14,
        out_specs=pl.BlockSpec(memory_space=pl.ANY),
        scratch_shapes=[
            pltpu.VMEM(((LANES + 8) * slots + 8, LANES), f32),
            pltpu.VMEM(((LEFT + 8) * (SPAN - 1), LANES), f32),
            pltpu.VMEM((LANES, LANES), f32),
            pltpu.VMEM((EDGE * groups, LANES), f32),
            pltpu.VMEM((EDGE * groups, LANES), f32),
            pltpu.VMEM((rows, LANES), f32),
            pltpu.VMEM((LANES, LANES), f32),
            pltpu.VMEM((slots, band, LANES), f32),
            pltpu.SemaphoreType.DMA((slots,)),
        ] + [pltpu.VMEM((LANES * LONG + 72, LANES), f32)] * (2 * SPAN),
        compiler_params=TIGHT,
        name="subtract",
    )(close(table), close(mine), close(scal_1), close(scal_2), close(scal_3), near(held), own, got_a, got_b, got_2, got_3,
      near(strip), halo_a, halo_t, halo_s, near(vec_0), near(vec_1), near(vec_2), near(vec_3))
    return out[None]


def solution(mesh):
    in_specs = (
        P("det", "row", None),
        P("det", None, "row", None),
        P(),
        P(None, "det", None),
        P(None, "det", None),
        P("det", None),
        P(),
        P("det", None),
        P("det"),
    )
    out_specs = P("det", None, "row", None)

    return jax.shard_map(body, mesh=mesh, in_specs=in_specs, out_specs=out_specs, check_vma=False)
```
